256 devices in a mesh: ens: 4 (over x), zero: 16 (over z, core), cols: 4 (over y).
Axes of the slice: x: 4, y: 4, z: 8, core: 2. Of those that a mesh axis runs over, the one named last changes fastest.
Arguments:
- one_gate: float32 [8192, 8192], P(('ens', 'zero'), 'cols'), parts along dimension 0, may hold values from -0.1875 to 0.1875
- other_gate: float32 [8192, 8192], P(('ens', 'zero'), 'cols'), parts along dimension 0, may hold values from -0.125 to 0.125
- one_up: float32 [8192, 8192], P(('ens', 'zero'), 'cols'), parts along dimension 0, may hold values from -0.1875 to 0.1875
- other_up: float32 [8192, 8192], P(('ens', 'zero'), 'cols'), parts along dimension 0, may hold values from -0.125 to 0.125
- mix_share: float32 [8192], P(('ens', 'zero')), parts along dimension 0, may hold values from 0.2 to 0.8
- norm_train: float32 [8192], P(('ens', 'zero', 'cols')), parts along dimension 0, may hold values from 0.25 to 1.75
- norm_step: float32 [8192], P(('ens', 'zero', 'cols')), parts along dimension 0, may hold values from -0.3 to 0.3
Outputs:
- serve_gate: bfloat16 [8192, 8192], P('ens', 'cols'), parts along dimension 0
- serve_up: bfloat16 [8192, 8192], P('ens', 'cols'), parts along dimension 0
- factor_gate: float32 [32768], P(('ens', 'cols')), parts along dimension 0
- factor_up: float32 [32768], P(('ens', 'cols')), parts along dimension 0
- serve_norm: bfloat16 [8192], P('ens'), parts along dimension 0
The draws below stay inside these ranges and needn't reach their ends.
There are 4 independent parts, one for each index of `ens`. The reference program is written for one: setup_inputs(seed, part) draws one part's arguments, and reference() takes and returns one part's arrays. A program takes and returns all parts, laid end to end along the dimension named above; each array names one. Nothing has to cross between parts.
All inputs are finite; a program needn't handle non-finite values. Where the reference program divides by a largest or mean magnitude, that divisor is 1e-20 or more.
Results may differ from the reference program's by a relative error of at most 0.001.
Values may be sent and summed in bfloat16 or wider, within the bound.
No kernel may reach another device: no remote copies, remote signals or barrier semaphores. Data moves between devices by JAX's collectives and lax.ppermute only.
A program may use at most 128 MiB of HBM per device.

```python
import jax
import jax.numpy as jnp

D_MODEL = 2048
D_INNER = 8192


def with_spikes(values, key, source, target, parts, factor):
    owner, partner = [(jnp.arange(values.shape[axis_at]) // (values.shape[axis_at] // parts)).reshape([-1 if axis == axis_at else 1 for axis in range(values.ndim)]) for axis_at in (source, target)]
    chosen = jax.random.permutation(key, parts)[partner]
    strong = (owner == chosen) | (owner == (partner + parts // 2) % parts)
    return jnp.where(strong, factor * values, values)


def levels(rng, extent, split, least, high):
    level = 1.0
    for axis_at, shards_of in split:
        heights = jax.random.uniform(jax.random.fold_in(jax.random.fold_in(rng, 6), axis_at), (shards_of,), jnp.float32, least / len(split), high / len(split))
        level = level * jnp.repeat(jnp.exp(heights), extent[axis_at] // shards_of).reshape((-1,) + (1,) * (len(extent) - 1 - axis_at))
    return level


def centred(stream_key, extent, deviation, bound, cuts=(), held_as=jnp.bfloat16):
    factor_of = levels(stream_key, extent, cuts, -0.22, 0.18) if cuts else 1.0
    entries = jax.random.normal(stream_key, extent, jnp.float32) * deviation * factor_of
    return jnp.minimum(jnp.maximum(entries, -bound), bound).astype(held_as)


def bell_draw_with(rng, extent, scale, limit, split, heavy, held_as=jnp.bfloat16):
    drawn = scale * jax.random.normal(rng, extent, jnp.float32)
    if split:
        drawn = drawn * levels(rng, extent, split, -0.22, 0.18)
    return jnp.clip(with_spikes(drawn, jax.random.fold_in(rng, 3), *heavy), -limit, limit).astype(held_as)


def setup_inputs(seed: int = 0, part: int = 0) -> dict:
    streams_of = jax.random.split(jax.random.key(seed), 8)
    part_splits = jax.random.split(jax.random.fold_in(streams_of[7], part), 8)
    one_gate = bell_draw_with(part_splits[0], (D_MODEL, D_INNER), D_MODEL ** -0.5, 0.1875, ((0, 16), (1, 4)), (0, 1, 16, 2.0), jnp.float32)
    other_gate = centred(part_splits[1], (D_MODEL, D_INNER), D_MODEL ** -0.5, 0.125, ((0, 16), (1, 4)), jnp.float32)
    one_up = bell_draw_with(part_splits[2], (D_MODEL, D_INNER), D_MODEL ** -0.5, 0.1875, ((0, 16), (1, 4)), (0, 1, 16, 2.0), jnp.float32)
    other_up = centred(part_splits[3], (D_MODEL, D_INNER), D_MODEL ** -0.5, 0.125, ((0, 16), (1, 4)), jnp.float32)
    mix_share = jnp.clip(0.2 + 0.6 * jax.random.uniform(part_splits[4], (D_MODEL,), jnp.float32) ** levels(part_splits[4], (D_MODEL,), ((0, 16),), -0.2, 0.2), 0.2, 0.8)
    norm_train = jnp.clip(1.0 + 0.15 * jax.random.normal(part_splits[5], (D_MODEL,), jnp.float32), 0.25, 1.75)
    norm_step = jnp.clip(jax.random.uniform(part_splits[6], (D_MODEL,), jnp.float32, -0.3, 0.3) * levels(part_splits[6], (D_MODEL,), ((0, 64),), -0.4, 0.0), -0.3, 0.3)
    return {"one_gate": one_gate, "other_gate": other_gate, "one_up": one_up, "other_up": other_up, "mix_share": mix_share, "norm_train": norm_train, "norm_step": norm_step}


def reference(one_gate, other_gate, one_up, other_up, mix_share, norm_train, norm_step):
    fresh_gate = mix_share[:, None] * one_gate + (1.0 - mix_share[:, None]) * other_gate
    fresh_up = mix_share[:, None] * one_up + (1.0 - mix_share[:, None]) * other_up
    factor_gate = jnp.sum(jnp.abs(fresh_gate), axis=0) / D_MODEL
    serve_gate = (fresh_gate / factor_gate).astype(jnp.bfloat16)
    factor_up = jnp.sum(jnp.abs(fresh_up), axis=0) / D_MODEL
    serve_up = (fresh_up / factor_up).astype(jnp.bfloat16)
    serve_norm = (norm_train + norm_step).astype(jnp.bfloat16)
    return serve_gate, serve_up, factor_gate, factor_up, serve_norm
```

```python
import jax
import jax.numpy as jnp
from jax import lax
from jax.sharding import PartitionSpec as P

D_MODEL = 2048
CHIPS = 8


def shift(x, by):
    perm = [(2 * z + c, 2 * ((z + by) % CHIPS) + c) for z in range(CHIPS) for c in range(2)]
    return lax.ppermute(x, "zero", perm)


def swap(x):
    return lax.ppermute(x, "zero", [(i, i ^ 1) for i in range(2 * CHIPS)])


def put(out, block, at):
    return lax.dynamic_update_slice(out, block, (at * block.shape[0], 0))


def gathered(block, plus, minus):
    me = lax.axis_index("zero")
    z, c = me >> 1, me & 1
    out = jnp.zeros((2 * CHIPS * block.shape[0], block.shape[1]), block.dtype)
    out = put(out, block, me)
    out = put(out, swap(block), me ^ 1)
    up, down = block, block
    for s in range(1, max(plus, minus) + 1):
        if s <= plus:
            up = shift(up, 1)
            src = (z - s) & (CHIPS - 1)
            out = put(out, up, 2 * src + c)
            out = put(out, swap(up), 2 * src + 1 - c)
        if s <= minus:
            down = shift(down, -1)
            src = (z + s) & (CHIPS - 1)
            out = put(out, down, 2 * src + c)
            out = put(out, swap(down), 2 * src + 1 - c)
    return out


def local(one_gate, other_gate, one_up, other_up, mix_share, norm_train, norm_step):
    share = mix_share[:, None]
    fresh_gate = share * one_gate + (1.0 - share) * other_gate
    fresh_up = share * one_up + (1.0 - share) * other_up
    sums = jnp.concatenate([jnp.sum(jnp.abs(fresh_gate), axis=0), jnp.sum(jnp.abs(fresh_up), axis=0)])
    everyone = lax.all_to_all(jnp.broadcast_to(sums[None], (16, sums.size)), "zero", 0, 0, tiled=True)
    factor = everyone.sum(axis=0) / D_MODEL
    factor_gate, factor_up = factor[:2048], factor[2048:]
    narrow_gate = (fresh_gate / factor_gate).astype(jnp.bfloat16)
    narrow_up = (fresh_up / factor_up).astype(jnp.bfloat16)
    serve_gate = gathered(narrow_gate, 4, 3)
    serve_up = gathered(narrow_up, 3, 4)
    norm = (norm_train + norm_step).astype(jnp.bfloat16)
    serve_norm = lax.all_to_all(jnp.broadcast_to(norm[None], (64, norm.size)), ("zero", "cols"), 0, 0, tiled=True).reshape(-1)
    return serve_gate, serve_up, factor_gate, factor_up, serve_norm


def solution(mesh):
    return jax.shard_map(
        local, mesh=mesh,
        in_specs=(P(("ens", "zero"), "cols"),) * 4 + (P(("ens", "zero")),) + (P(("ens", "zero", "cols")),) * 2,
        out_specs=(P("ens", "cols"), P("ens", "cols"), P(("ens", "cols")), P(("ens", "cols")), P("ens")),
        check_vma=False,
    )
```
